32 devices in a mesh: row: 8 (over z, y), ma: 4 (over x, core).
Axes of the slice: x: 2, y: 2, z: 4, core: 2. Of those that a mesh axis runs over, the one named last changes fastest.
Arguments:
- thermal_state: float32 [64, 768, 2048], P('row', None, 'ma'), may hold values from -6 to 6
- sphere_node_annulus: int32 [64, 768], P('row'), may hold values from 0 to 1022, as said below
- sphere_node_offset: float32 [64, 768], P('row'), may hold values from 0 to 1
- integration_share: float32 [64, 768], P('row'), may hold values from 0.02 to 0.2
- annulus_holder_row: int32 [1024], replicated, may hold values from 0 to 7, never falling along the last dimension, each value on 1 to 256 neighbouring positions
- rotating_flow_potential: float32 [2048, 2048], P('row', 'ma'), may hold values from -6 to 6
Outputs:
- thermal_state_later: float32 [64, 768, 2048], P('row', None, 'ma')
- flow_potential_later: float32 [2048, 2048], P('row', 'ma')
The draws below stay inside these ranges and needn't reach their ends.
Inputs may be any that keep to these rules, and one draw needn't show every extreme that they name: `sphere_node_annulus`: lower cell of each point; the next cell exists. `annulus_holder_row`: never falling along cells; each owner holds 1 to 256 cells and some owner exactly 256.
All inputs are finite; a program needn't handle non-finite values.
Results may differ from the reference program's by a relative error of at most 0.0003.
Values sent between devices are 32-bit elements; how exact they have to be, the bound alone decides.
A program may use at most 64 MiB of HBM per device.

```python
import math
import jax
import jax.numpy as jnp
import numpy as np
from jax import lax

NS = 1024
LONGITUDE_NODES = 2048
MERIDIAN_NODES = 768
SPHERE_LEVELS = 64
S_MOST = 256
OWNER_SLOTS = 2048
N_ROW = 8


def draw_sphere_node_annulus(key, part):
    centre_distance = jnp.arange(SPHERE_LEVELS, dtype=jnp.int32)[:, None]
    colatitude = jnp.arange(MERIDIAN_NODES, dtype=jnp.int32)[None, :]
    inner_radius = 7 * SPHERE_LEVELS // 13
    sine_level = 4 * (colatitude + 1) * (MERIDIAN_NODES - colatitude) * 1024 // ((MERIDIAN_NODES + 1) * (MERIDIAN_NODES + 1))
    column_base = (inner_radius + centre_distance) * sine_level * (NS - 2) // ((inner_radius + SPHERE_LEVELS) * 1024)
    jitter = jax.random.randint(key, (SPHERE_LEVELS, MERIDIAN_NODES), -1, 2, dtype=jnp.int32)
    return jnp.clip(column_base + jitter, 0, NS - 2).astype(jnp.int32)


def levels(key, shape, pieces, least, high):
    level = 1.0
    for dim, shards_of in pieces:
        draws = jax.random.uniform(jax.random.fold_in(jax.random.fold_in(key, 6), dim), (shards_of,), jnp.float32, least / len(pieces), high / len(pieces))
        level = level * jnp.repeat(jnp.exp(draws), shape[dim] // shards_of).reshape((-1,) + (1,) * (len(shape) - 1 - dim))
    return level


def length_profile(number_of, total, reach, lean):
    portions = [(1 << 20) // math.isqrt(grade ** lean) + 1 for grade in range(2, number_of + 1)]
    surplus, counts = total - reach - (number_of - 1), [1] * (number_of - 1)
    while surplus > 0:
        candidates = [i for i in range(number_of - 1) if counts[i] < reach]
        whole, budget = sum([portions[i] for i in candidates]), surplus
        for i in candidates:
            extra = min(reach - counts[i], max(1, budget * portions[i] // whole), surplus)
            counts[i] = counts[i] + extra
            surplus = surplus - extra
    return np.array([reach] + counts)


def uneven_parts(stream_key, amount, total, bound, skew):
    if amount == 2:
        one = jax.random.randint(stream_key, (), max(1, total - bound), min(bound, total - 1) + 1)
        return jnp.stack([one, total - one])
    sizes = jnp.asarray(length_profile(amount, total, bound, skew), jnp.int32)
    pairs = (amount - 1) // 2
    donor, taker = sizes[1:1 + 2 * pairs:2], sizes[2:2 + 2 * pairs:2]
    margin = jnp.minimum(donor - 1, bound - taker)
    passed = jax.random.randint(jax.random.fold_in(stream_key, 1), (pairs,), 0, 1 << 20) % (margin + 1)
    sizes = sizes.at[1:1 + 2 * pairs:2].set(donor - passed).at[2:2 + 2 * pairs:2].set(taker + passed)
    return sizes[jax.random.permutation(jax.random.fold_in(stream_key, 2), amount)]


def normal_values(rng, shape, spread, reach, shards=(), held_as=jnp.bfloat16):
    result = jax.random.normal(rng, shape, jnp.float32) * spread
    if len(shards) > 0:
        result = levels(rng, shape, shards, -0.22, 0.18) * result
    return jnp.clip(result, min=-reach, max=reach).astype(held_as)


def setup_inputs(seed: int = 0) -> dict:
    seeds = jax.random.split(jax.random.key(seed), 7)
    thermal_state = normal_values(seeds[0], (SPHERE_LEVELS, MERIDIAN_NODES, LONGITUDE_NODES), 1.0, 6.0, ((0, 8), (2, 4)), jnp.float32)
    sphere_node_annulus = draw_sphere_node_annulus(jax.random.fold_in(seeds[6], 71), 0)
    sphere_node_offset = jnp.clip(1.0 * jax.random.uniform(seeds[2], (SPHERE_LEVELS, MERIDIAN_NODES), jnp.float32) ** levels(seeds[2], (SPHERE_LEVELS, MERIDIAN_NODES), ((0, 8),), -0.2, 0.2), 0.0, 1.0)
    integration_share = jnp.clip(jnp.exp(math.log(0.2) - 2.3025851 * jax.random.uniform(seeds[3], (SPHERE_LEVELS, MERIDIAN_NODES), jnp.float32) ** levels(seeds[3], (SPHERE_LEVELS, MERIDIAN_NODES), ((0, 8),), -0.2, 0.2)), 0.02, 0.2)
    annulus_holder_row = jnp.searchsorted(jnp.cumsum(uneven_parts(seeds[4], N_ROW, NS, S_MOST, 2)), jnp.arange(NS), side="right").astype(jnp.int32)
    rotating_flow_potential = normal_values(seeds[5], (OWNER_SLOTS, LONGITUDE_NODES), 1.0, 6.0, ((0, 8), (1, 4)), jnp.float32)
    return dict(thermal_state=thermal_state, sphere_node_annulus=sphere_node_annulus, sphere_node_offset=sphere_node_offset, integration_share=integration_share, annulus_holder_row=annulus_holder_row, rotating_flow_potential=rotating_flow_potential)


stream_step = 0.5
thermal_advance = 0.25


def reference(thermal_state, sphere_node_annulus, sphere_node_offset, integration_share, annulus_holder_row, rotating_flow_potential):
    cells = jnp.arange(NS, dtype=jnp.int32)
    before = jnp.sum((annulus_holder_row[None, :] < annulus_holder_row[:, None]).astype(jnp.int32), axis=1)
    slot_of_cell = (annulus_holder_row * S_MOST + cells - before).astype(jnp.int32)
    geo = 1.0 / (0.25 + (cells.astype(jnp.float32) + 0.5) / NS)
    below_share = integration_share * (1.0 - sphere_node_offset)
    above_share = integration_share * sphere_node_offset

    def accumulate(total, items):
        plane, lower, low_w, high_w = items
        total = total + jax.ops.segment_sum(low_w[:, None] * plane, lower, num_segments=NS)
        total = total + jax.ops.segment_sum(high_w[:, None] * plane, lower + 1, num_segments=NS)
        return total, None

    zint, _ = lax.scan(accumulate, jnp.zeros((NS, LONGITUDE_NODES), jnp.float32),
                       (thermal_state, sphere_node_annulus, below_share, above_share))
    forcing = -geo[:, None] * ((jnp.roll(zint, -1, 1) - jnp.roll(zint, 1, 1)) * 0.5)
    stream_cell = rotating_flow_potential[slot_of_cell] + stream_step * forcing
    flow_potential_later = rotating_flow_potential.at[slot_of_cell].set(stream_cell)
    velocity = geo[:, None] * ((jnp.roll(stream_cell, -1, 1) - jnp.roll(stream_cell, 1, 1)) * 0.5)
    angle = math.pi * (jnp.arange(MERIDIAN_NODES, dtype=jnp.float32) + 0.5) / MERIDIAN_NODES
    sin_theta_term = jnp.sin(angle)[:, None]
    cos_theta_term = jnp.cos(angle)[:, None]

    def march_forward(centre_distance):
        present_entry = thermal_state[centre_distance]
        preceding_entry = jnp.where(centre_distance > 0, thermal_state[jnp.maximum(centre_distance - 1, 0)], 0.0)
        successor_entry = jnp.where(centre_distance < SPHERE_LEVELS - 1, thermal_state[jnp.minimum(centre_distance + 1, SPHERE_LEVELS - 1)], 0.0)
        distance_from_centre = (successor_entry - preceding_entry) * 0.5
        wrapped_heat_grid = jnp.pad(present_entry, ((1, 1), (0, 0)))
        theta_from_north = (wrapped_heat_grid[2:] - wrapped_heat_grid[:-2]) * 0.5
        lower = sphere_node_annulus[centre_distance]
        fraction = sphere_node_offset[centre_distance][:, None]
        shifted_heat = (1.0 - fraction) * velocity[lower] + fraction * velocity[lower + 1]
        return present_entry - thermal_advance * shifted_heat * (sin_theta_term * distance_from_centre + cos_theta_term * theta_from_north)

    thermal_state_later = lax.map(march_forward, jnp.arange(SPHERE_LEVELS, dtype=jnp.int32))
    return thermal_state_later, flow_potential_later
```

```python
import functools
import math

import jax
import jax.numpy as jnp
from jax import lax
from jax.experimental import pallas as pl
from jax.experimental.pallas import tpu as pltpu
from jax.sharding import PartitionSpec as P

stream_step = 0.5
thermal_advance = 0.25
WINDOW = 256
STRIP = 32
LANES = 128


def split(x):
    high = x.astype(jnp.bfloat16)
    return high, (x - high.astype(jnp.float32)).astype(jnp.bfloat16)


def dot3(a_high, a_low, b_high, b_low):
    dot = functools.partial(jnp.dot, preferred_element_type=jnp.float32)
    return dot(a_high, b_high) + (dot(a_high, b_low) + dot(a_low, b_high))


def as_column(row):
    return jnp.broadcast_to(row, (LANES, row.shape[1])).T


def azimuth_difference(x, before, after, lanes):
    width = x.shape[1]
    left = jnp.where(lanes == 0, before, pltpu.roll(x, 1, 1))
    right = jnp.where(lanes == width - 1, after, pltpu.roll(x, width - 1, 1))
    return right - left


def geo_of(first, rows, cells):
    c = lax.broadcasted_iota(jnp.int32, (rows, 1), 0) + first
    return 1.0 / (0.25 + (c.astype(jnp.float32) + 0.5) / cells)


def integral_kernel(start, wins, t_ref, a_ref, f_ref, q_ref, z_ref, first_ref, last_ref, acc):
    i = pl.program_id(0)
    cells, width = z_ref.shape

    @pl.when(i == 0)
    def _():
        acc[...] = jnp.zeros_like(acc)

    t_high, t_low = split(t_ref[...].reshape(-1, width))
    a, f, q = a_ref[0], f_ref[0], q_ref[0]
    b_high, b_low = split(q * (1.0 - f))
    c_high, c_low = split(q * f)
    b_high, b_low, c_high, c_low = (x.astype(jnp.float32) for x in (b_high, b_low, c_high, c_low))
    row = lax.broadcasted_iota(jnp.int32, (WINDOW, a.shape[1]), 0)

    def window(k, carry):
        s = pl.multiple_of(start[i] + k * WINDOW, 16)
        d = row - (a - s)
        low, high = d == 0, d == 1
        w_high = jnp.where(low, b_high, jnp.where(high, c_high, 0.0)).astype(jnp.bfloat16)
        w_low = jnp.where(low, b_low, jnp.where(high, c_low, 0.0)).astype(jnp.bfloat16)
        acc[pl.ds(s, WINDOW), :] += dot3(w_high, w_low, t_high, t_low)
        return carry

    lax.fori_loop(0, wins[i], window, 0)

    @pl.when(i == pl.num_programs(0) - 1)
    def _():
        z_ref[...] = acc[0:cells, :]
        first_ref[...] = acc[0:cells, 0:LANES].T[0:8]
        last_ref[...] = acc[0:cells, width - LANES:width].T[LANES - 8:LANES]


def stream_kernel(own, z_ref, hb_ref, ha_ref, pot_ref, u_ref, pad):
    cells, width = z_ref.shape
    slots = pot_ref.shape[0]
    before, count = own[0], own[1]
    pad[cells:cells + slots, :] = pot_ref[...]
    lanes = lax.broadcasted_iota(jnp.int32, (LANES, width), 1)
    for c0 in range(0, cells, LANES):
        hb = as_column(hb_ref[7:8, c0:c0 + LANES])[:, 0:1]
        ha = as_column(ha_ref[0:1, c0:c0 + LANES])[:, 0:1]
        rows = slice(c0, c0 + LANES)
        diff = azimuth_difference(z_ref[rows, :], hb, ha, lanes)
        forcing = -geo_of(c0, LANES, cells) * (diff * 0.5)
        at = lax.broadcasted_iota(jnp.int32, (LANES, width), 0) + (c0 - before)
        from_row = cells + c0 - before
        tile = pl.multiple_of(from_row // 8 * 8, 8)
        held = pltpu.roll(pad[pl.ds(tile, LANES + 8), :], lax.rem(LANES + 8 - (from_row - tile), LANES + 8), 0)[:LANES]
        u_ref[rows, :] = stream_step * forcing + jnp.where((at >= 0) & (at < count), held, 0.0)


def advance_kernel(start, wins, g_ref, hb_ref, ha_ref, a_ref, f_ref, t_ref, up_ref, dn_ref,
                   in_ref, out_ref, sin_ref, cos_ref, o_ref, v_high, v_low, drift):
    i = pl.program_id(0)
    n = pl.num_programs(0)
    cells, width = g_ref.shape
    radii, strip, _ = t_ref.shape

    @pl.when(i == 0)
    def _():
        lanes = lax.broadcasted_iota(jnp.int32, (LANES, width), 1)
        for c0 in range(0, cells, LANES):
            rows = slice(c0, c0 + LANES)
            hb = as_column(hb_ref[7:8, rows])[:, 0:1]
            ha = as_column(ha_ref[0:1, rows])[:, 0:1]
            diff = azimuth_difference(g_ref[rows, :], hb, ha, lanes)
            high, low = split(geo_of(c0, LANES, cells) * (diff * 0.5))
            v_high[rows, :] = high
            v_low[rows, :] = low
        v_high[cells:, :] = jnp.zeros((v_high.shape[0] - cells, width), jnp.bfloat16)
        v_low[cells:, :] = jnp.zeros((v_low.shape[0] - cells, width), jnp.bfloat16)

    a = as_column(a_ref[0])
    f = as_column(f_ref[0])
    b_high, b_low = (x.astype(jnp.float32) for x in split(1.0 - f))
    c_high, c_low = (x.astype(jnp.float32) for x in split(f))
    lane = lax.broadcasted_iota(jnp.int32, a.shape, 1).astype(jnp.float32) - a
    drift[...] = jnp.zeros_like(drift)

    def window(k, carry):
        s = pl.multiple_of(start[i] + k * WINDOW, 16)
        highs, lows = [], []
        for h in range(0, WINDOW, LANES):
            d = lane + (s + h).astype(jnp.float32)
            low, high = d == 0.0, d == 1.0
            highs.append(jnp.where(low, b_high, jnp.where(high, c_high, 0.0)).astype(jnp.bfloat16))
            lows.append(jnp.where(low, b_low, jnp.where(high, c_low, 0.0)).astype(jnp.bfloat16))
        here = pl.ds(s, WINDOW)
        drift[...] += dot3(
            jnp.concatenate(highs, 1), jnp.concatenate(lows, 1), v_high[here, :], v_low[here, :]
        )
        return carry

    lax.fori_loop(0, wins[i], window, 0)

    tt = lax.broadcasted_iota(jnp.int32, (strip, width), 0)
    sine, cosine = sin_ref[...] * 0.5, cos_ref[...] * 0.5
    north_there = (i > 0).astype(jnp.float32)
    south_there = (i < n - 1).astype(jnp.float32)
    for r in range(radii):
        t = t_ref[r]
        inner = t_ref[r - 1] if r > 0 else in_ref[0]
        outer = t_ref[r + 1] if r < radii - 1 else out_ref[0]
        north = jnp.where(tt == 0, up_ref[r, 7:8, :] * north_there, pltpu.roll(t, 1, 0))
        south = jnp.where(tt == strip - 1, dn_ref[r, 0:1, :] * south_there, pltpu.roll(t, strip - 1, 0))
        slope = sine * (outer - inner) + cosine * (south - north)
        o_ref[r] = t - thermal_advance * drift[r * strip:(r + 1) * strip, :] * slope


def per_device(thermal, annulus, offset, share, holder, pot):
    radii, meridian, width = thermal.shape
    slots, cells = pot.shape[0], holder.shape[0]
    row = lax.axis_index("row")
    n_row, n_ma = lax.axis_size("row"), lax.axis_size("ma")
    count = meridian // STRIP
    points = radii * STRIP

    row_up = [(i, i + 1) for i in range(n_row - 1)]
    inner = lax.ppermute(thermal[-1:], "row", row_up)
    outer = lax.ppermute(thermal[:1], "row", [(j, i) for i, j in row_up])

    def arrange(x):
        return x.reshape(radii, count, STRIP).transpose(1, 0, 2).reshape(count, 1, points)

    a = arrange(annulus)
    f = arrange(offset)
    q = arrange(share)
    start = jnp.min(a, axis=(1, 2)) // 16 * 16
    wins = (jnp.max(a, axis=(1, 2)) + 1 - start) // WINDOW + 1
    own = jnp.stack([jnp.sum((holder < row).astype(jnp.int32)),
                     jnp.sum((holder == row).astype(jnp.int32))])

    small = pl.BlockSpec((1, 1, points), lambda i, *_: (i, 0, 0))
    slab = pl.BlockSpec((radii, STRIP, width), lambda i, *_: (0, i, 0))
    whole = lambda *shape: pl.BlockSpec(shape, lambda i, *_: (0,) * len(shape))
    f32 = lambda *shape: jax.ShapeDtypeStruct(shape, jnp.float32)
    flops = 6 * meridian * radii * WINDOW * width
    size = 4 * radii * meridian * width

    zint, first, last = pl.pallas_call(
        integral_kernel,
        grid_spec=pltpu.PrefetchScalarGridSpec(
            num_scalar_prefetch=2,
            grid=(count,),
            in_specs=[slab, small, small, small],
            out_specs=[whole(cells, width), whole(8, cells), whole(8, cells)],
            scratch_shapes=[pltpu.VMEM((cells + WINDOW, width), jnp.float32)],
        ),
        out_shape=[f32(cells, width), f32(8, cells), f32(8, cells)],
        cost_estimate=pl.CostEstimate(flops=flops, bytes_accessed=size, transcendentals=0),
        name="integral",
    )(start, wins, thermal, a, f, q)

    ma_up = [(i, (i + 1) % n_ma) for i in range(n_ma)]
    ma_down = [(j, i) for i, j in ma_up]
    stream = pl.pallas_call(
        stream_kernel,
        in_specs=[pl.BlockSpec(memory_space=pltpu.SMEM)] + [pl.BlockSpec(memory_space=pltpu.VMEM)] * 4,
        out_specs=pl.BlockSpec(memory_space=pltpu.VMEM),
        scratch_shapes=[pltpu.VMEM((2 * cells + LANES, width), jnp.float32)],
        out_shape=f32(cells, width),
        cost_estimate=pl.CostEstimate(flops=8 * cells * width, bytes_accessed=16 * cells * width, transcendentals=0),
        name="stream",
    )(own, zint, lax.ppermute(last, "ma", ma_up), lax.ppermute(first, "ma", ma_down), pot)

    stream = lax.psum_scatter(stream, "row", scatter_dimension=0, tiled=True)
    stream = lax.all_gather(stream, "row", axis=0, tiled=True)

    mine = lax.dynamic_slice(jnp.pad(stream, ((0, slots), (0, 0))), (own[0], 0), (slots, width))
    pot_later = jnp.where(jnp.arange(slots)[:, None] < own[1], mine, pot)
    first = jnp.broadcast_to(stream[:, 0][None, :], (8, cells))
    last = jnp.broadcast_to(stream[:, -1][None, :], (8, cells))
    angle = math.pi * (jnp.arange(meridian, dtype=jnp.float32) + 0.5) / meridian

    step = STRIP // 8
    ends = meridian // 8 - 1
    thermal_later = pl.pallas_call(
        advance_kernel,
        grid_spec=pltpu.PrefetchScalarGridSpec(
            num_scalar_prefetch=2,
            grid=(count,),
            in_specs=[
                whole(cells, width), whole(8, cells), whole(8, cells), small, small, slab,
                pl.BlockSpec((radii, 8, width), lambda i, *_: (0, jnp.maximum(i * step - 1, 0), 0)),
                pl.BlockSpec((radii, 8, width), lambda i, *_: (0, jnp.minimum(i * step + step, ends), 0)),
                pl.BlockSpec((1, STRIP, width), lambda i, *_: (0, i, 0)),
                pl.BlockSpec((1, STRIP, width), lambda i, *_: (0, i, 0)),
                pl.BlockSpec((STRIP, 1), lambda i, *_: (i, 0)),
                pl.BlockSpec((STRIP, 1), lambda i, *_: (i, 0)),
            ],
            out_specs=slab,
            scratch_shapes=[
                pltpu.VMEM((cells + WINDOW, width), jnp.bfloat16),
                pltpu.VMEM((cells + WINDOW, width), jnp.bfloat16),
                pltpu.VMEM((points, width), jnp.float32),
            ],
        ),
        out_shape=f32(radii, meridian, width),
        cost_estimate=pl.CostEstimate(flops=flops, bytes_accessed=2 * size, transcendentals=0),
        name="advance",
    )(start, wins, stream, lax.ppermute(last, "ma", ma_up), lax.ppermute(first, "ma", ma_down),
      a.astype(jnp.float32), f, thermal, thermal, thermal, inner, outer,
      jnp.sin(angle)[:, None], jnp.cos(angle)[:, None])
    return thermal_later, pot_later


def solution(mesh):
    return jax.shard_map(
        per_device,
        mesh=mesh,
        in_specs=(
            P("row", None, "ma"),
            P("row", None),
            P("row", None),
            P("row", None),
            P(),
            P("row", "ma"),
        ),
        out_specs=(P("row", None, "ma"), P("row", "ma")),
        check_vma=False,
    )
```

```python
import functools
import math

import jax
import jax.numpy as jnp
from jax import lax
from jax.experimental import pallas as pl
from jax.experimental.pallas import tpu as pltpu
from jax.sharding import PartitionSpec as P

stream_step = 0.5
thermal_advance = 0.25
WINDOW = 256
STRIP = 32
LANES = 128


def split(x):
    high = x.astype(jnp.bfloat16)
    return high, (x - high.astype(jnp.float32)).astype(jnp.bfloat16)


def dot3(a_high, a_low, b_high, b_low):
    dot = functools.partial(jnp.dot, preferred_element_type=jnp.float32)
    return dot(a_high, b_high) + (dot(a_high, b_low) + dot(a_low, b_high))


def as_column(row):
    return jnp.broadcast_to(row, (LANES, row.shape[1])).T


def azimuth_difference(x, before, after, lanes):
    width = x.shape[1]
    left = jnp.where(lanes == 0, before, pltpu.roll(x, 1, 1))
    right = jnp.where(lanes == width - 1, after, pltpu.roll(x, width - 1, 1))
    return right - left


def geo_of(first, rows, cells):
    c = lax.broadcasted_iota(jnp.int32, (rows, 1), 0) + first
    return 1.0 / (0.25 + (c.astype(jnp.float32) + 0.5) / cells)


def integral_kernel(start, wins, t_ref, a_ref, f_ref, q_ref, z_ref, first_ref, last_ref, acc):
    i = pl.program_id(0)
    cells, width = z_ref.shape

    @pl.when(i == 0)
    def _():
        acc[...] = jnp.zeros_like(acc)

    t_high, t_low = split(t_ref[...].reshape(-1, width))
    a, f, q = a_ref[0], f_ref[0], q_ref[0]
    b_high, b_low = split(q * (1.0 - f))
    c_high, c_low = split(q * f)
    b_high, b_low, c_high, c_low = (x.astype(jnp.float32) for x in (b_high, b_low, c_high, c_low))
    row = lax.broadcasted_iota(jnp.int32, (WINDOW, a.shape[1]), 0)

    def window(k, carry):
        s = pl.multiple_of(start[i] + k * WINDOW, 16)
        d = row - (a - s)
        low, high = d == 0, d == 1
        w_high = jnp.where(low, b_high, jnp.where(high, c_high, 0.0)).astype(jnp.bfloat16)
        w_low = jnp.where(low, b_low, jnp.where(high, c_low, 0.0)).astype(jnp.bfloat16)
        acc[pl.ds(s, WINDOW), :] += dot3(w_high, w_low, t_high, t_low)
        return carry

    lax.fori_loop(0, wins[i], window, 0)

    @pl.when(i == pl.num_programs(0) - 1)
    def _():
        z_ref[...] = acc[0:cells, :]
        first_ref[...] = acc[0:cells, 0:LANES].T[0:8]
        last_ref[...] = acc[0:cells, width - LANES:width].T[LANES - 8:LANES]


def stream_kernel(own, z_ref, hb_ref, ha_ref, pot_ref, u_ref, pad):
    cells, width = z_ref.shape
    slots = pot_ref.shape[0]
    before, count = own[0], own[1]
    pad[cells:cells + slots, :] = pot_ref[...]
    lanes = lax.broadcasted_iota(jnp.int32, (LANES, width), 1)
    for c0 in range(0, cells, LANES):
        hb = as_column(hb_ref[7:8, c0:c0 + LANES])[:, 0:1]
        ha = as_column(ha_ref[0:1, c0:c0 + LANES])[:, 0:1]
        rows = slice(c0, c0 + LANES)
        diff = azimuth_difference(z_ref[rows, :], hb, ha, lanes)
        forcing = -geo_of(c0, LANES, cells) * (diff * 0.5)
        at = lax.broadcasted_iota(jnp.int32, (LANES, width), 0) + (c0 - before)
        from_row = cells + c0 - before
        tile = pl.multiple_of(from_row // 8 * 8, 8)
        held = pltpu.roll(pad[pl.ds(tile, LANES + 8), :], lax.rem(LANES + 8 - (from_row - tile), LANES + 8), 0)[:LANES]
        u_ref[rows, :] = stream_step * forcing + jnp.where((at >= 0) & (at < count), held, 0.0)


def advance_kernel(start, wins, g_ref, hb_ref, ha_ref, a_ref, f_ref, t_ref, up_ref, dn_ref,
                   in_ref, out_ref, sin_ref, cos_ref, o_ref, v_high, v_low, drift):
    i = pl.program_id(0)
    n = pl.num_programs(0)
    cells, width = g_ref.shape
    radii, strip, _ = t_ref.shape

    @pl.when(i == 0)
    def _():
        lanes = lax.broadcasted_iota(jnp.int32, (LANES, width), 1)
        for c0 in range(0, cells, LANES):
            rows = slice(c0, c0 + LANES)
            hb = as_column(hb_ref[7:8, rows])[:, 0:1]
            ha = as_column(ha_ref[0:1, rows])[:, 0:1]
            diff = azimuth_difference(g_ref[rows, :], hb, ha, lanes)
            high, low = split(geo_of(c0, LANES, cells) * (diff * 0.5))
            v_high[rows, :] = high
            v_low[rows, :] = low
        v_high[cells:, :] = jnp.zeros((v_high.shape[0] - cells, width), jnp.bfloat16)
        v_low[cells:, :] = jnp.zeros((v_low.shape[0] - cells, width), jnp.bfloat16)

    a = as_column(a_ref[0])
    f = as_column(f_ref[0])
    b_high, b_low = (x.astype(jnp.float32) for x in split(1.0 - f))
    c_high, c_low = (x.astype(jnp.float32) for x in split(f))
    lane = lax.broadcasted_iota(jnp.int32, a.shape, 1).astype(jnp.float32) - a
    drift[...] = jnp.zeros_like(drift)

    def window(k, carry):
        s = pl.multiple_of(start[i] + k * WINDOW, 16)
        highs, lows = [], []
        for h in range(0, WINDOW, LANES):
            d = lane + (s + h).astype(jnp.float32)
            low, high = d == 0.0, d == 1.0
            highs.append(jnp.where(low, b_high, jnp.where(high, c_high, 0.0)).astype(jnp.bfloat16))
            lows.append(jnp.where(low, b_low, jnp.where(high, c_low, 0.0)).astype(jnp.bfloat16))
        here = pl.ds(s, WINDOW)
        drift[...] += dot3(
            jnp.concatenate(highs, 1), jnp.concatenate(lows, 1), v_high[here, :], v_low[here, :]
        )
        return carry

    lax.fori_loop(0, wins[i], window, 0)

    tt = lax.broadcasted_iota(jnp.int32, (strip, width), 0)
    sine, cosine = sin_ref[...] * 0.5, cos_ref[...] * 0.5
    north_there = (i > 0).astype(jnp.float32)
    south_there = (i < n - 1).astype(jnp.float32)
    for r in range(radii):
        t = t_ref[r]
        inner = t_ref[r - 1] if r > 0 else in_ref[0]
        outer = t_ref[r + 1] if r < radii - 1 else out_ref[0]
        north = jnp.where(tt == 0, up_ref[r, 7:8, :] * north_there, pltpu.roll(t, 1, 0))
        south = jnp.where(tt == strip - 1, dn_ref[r, 0:1, :] * south_there, pltpu.roll(t, strip - 1, 0))
        slope = sine * (outer - inner) + cosine * (south - north)
        o_ref[r] = t - thermal_advance * drift[r * strip:(r + 1) * strip, :] * slope


def ring_kernel(n, u_ref, g_ref, got, total, send, recv):
    me = lax.axis_index("row")
    level, side = lax.div(me, 2), lax.rem(me, 2)
    place = level * (1 - side) + (n - 1 - level) * side

    def row_of(p):
        back = lax.div(p, n // 2)
        return 2 * (p * (1 - back) + (n - 1 - p) * back) + back

    partner = (row_of(lax.rem(place + 1, n)), row_of(lax.rem(place + n - 1, n)))
    mesh_id = pl.DeviceIdType.MESH
    barrier = pltpu.get_barrier_semaphore()
    for p in partner:
        pl.semaphore_signal(barrier, inc=1, device_id={"row": p}, device_id_type=mesh_id)
    pl.semaphore_wait(barrier, 2)

    part = u_ref.shape[0] // n
    half = part // 2

    def rows(steps, d):
        k = lax.rem(place + (2 * n - steps if d == 0 else steps), n)
        return pl.ds(pl.multiple_of(k * part + d * half, 8), half)

    def copy(s, d):
        if s == 0:
            source, target = u_ref.at[rows(1, d)], got.at[d, 0]
        elif s < n - 1:
            source, target = got.at[d, s - 1], got.at[d, s]
        else:
            source = target = total.at[rows(s - (n - 1), d)]
        return pltpu.make_async_remote_copy(
            src_ref=source, dst_ref=target, send_sem=send.at[d, s], recv_sem=recv.at[d, s],
            device_id={"row": partner[d]}, device_id_type=mesh_id,
        )

    copies = [[copy(s, d) for d in (0, 1)] for s in range(2 * (n - 1))]
    for d in (0, 1):
        copies[0][d].start()
    for s in range(2 * (n - 1)):
        for d in (0, 1):
            copies[s][d].wait_recv()
            if s < n - 2:
                got[d, s] = got[d, s] + u_ref[rows(s + 2, d), :]
            elif s == n - 2:
                total[rows(0, d), :] = got[d, s] + u_ref[rows(0, d), :]
            if s + 1 < 2 * (n - 1):
                copies[s + 1][d].start()
    for pair in copies:
        for d in (0, 1):
            pair[d].wait_send()
    g_ref[...] = total[...]


def per_device(thermal, annulus, offset, share, holder, pot):
    radii, meridian, width = thermal.shape
    slots, cells = pot.shape[0], holder.shape[0]
    row = lax.axis_index("row")
    n_row, n_ma = lax.axis_size("row"), lax.axis_size("ma")
    count = meridian // STRIP
    points = radii * STRIP

    row_up = [(i, i + 1) for i in range(n_row - 1)]
    inner = lax.ppermute(thermal[-1:], "row", row_up)
    outer = lax.ppermute(thermal[:1], "row", [(j, i) for i, j in row_up])

    def arrange(x):
        return x.reshape(radii, count, STRIP).transpose(1, 0, 2).reshape(count, 1, points)

    a = arrange(annulus)
    f = arrange(offset)
    q = arrange(share)
    start = jnp.min(a, axis=(1, 2)) // 16 * 16
    wins = (jnp.max(a, axis=(1, 2)) + 1 - start) // WINDOW + 1
    own = jnp.stack([jnp.sum((holder < row).astype(jnp.int32)),
                     jnp.sum((holder == row).astype(jnp.int32))])

    small = pl.BlockSpec((1, 1, points), lambda i, *_: (i, 0, 0))
    slab = pl.BlockSpec((radii, STRIP, width), lambda i, *_: (0, i, 0))
    whole = lambda *shape: pl.BlockSpec(shape, lambda i, *_: (0,) * len(shape))
    f32 = lambda *shape: jax.ShapeDtypeStruct(shape, jnp.float32)

    zint, first, last = pl.pallas_call(
        integral_kernel,
        grid_spec=pltpu.PrefetchScalarGridSpec(
            num_scalar_prefetch=2,
            grid=(count,),
            in_specs=[slab, small, small, small],
            out_specs=[whole(cells, width), whole(8, cells), whole(8, cells)],
            scratch_shapes=[pltpu.VMEM((cells + WINDOW, width), jnp.float32)],
        ),
        out_shape=[f32(cells, width), f32(8, cells), f32(8, cells)],
        name="integral",
    )(start, wins, thermal, a, f, q)

    ma_up = [(i, (i + 1) % n_ma) for i in range(n_ma)]
    ma_down = [(j, i) for i, j in ma_up]
    stream = pl.pallas_call(
        stream_kernel,
        in_specs=[pl.BlockSpec(memory_space=pltpu.SMEM)] + [pl.BlockSpec(memory_space=pltpu.VMEM)] * 4,
        out_specs=pl.BlockSpec(memory_space=pltpu.VMEM),
        scratch_shapes=[pltpu.VMEM((2 * cells + LANES, width), jnp.float32)],
        out_shape=f32(cells, width),
        name="stream",
    )(own, zint, lax.ppermute(last, "ma", ma_up), lax.ppermute(first, "ma", ma_down), pot)

    part = cells // n_row // 2
    stream = pl.pallas_call(
        functools.partial(ring_kernel, n_row),
        in_specs=[pl.BlockSpec(memory_space=pltpu.VMEM)],
        out_specs=pl.BlockSpec(memory_space=pltpu.VMEM),
        scratch_shapes=[
            pltpu.VMEM((2, n_row - 1, part, width), jnp.float32),
            pltpu.VMEM((cells, width), jnp.float32),
            pltpu.SemaphoreType.DMA((2, 2 * (n_row - 1))),
            pltpu.SemaphoreType.DMA((2, 2 * (n_row - 1))),
        ],
        out_shape=f32(cells, width),
        compiler_params=pltpu.CompilerParams(collective_id=0, has_side_effects=True),
        name="ring",
    )(stream)

    mine = lax.dynamic_slice(jnp.pad(stream, ((0, slots), (0, 0))), (own[0], 0), (slots, width))
    pot_later = jnp.where(jnp.arange(slots)[:, None] < own[1], mine, pot)
    first = jnp.broadcast_to(stream[:, 0][None, :], (8, cells))
    last = jnp.broadcast_to(stream[:, -1][None, :], (8, cells))
    angle = math.pi * (jnp.arange(meridian, dtype=jnp.float32) + 0.5) / meridian

    step = STRIP // 8
    ends = meridian // 8 - 1
    thermal_later = pl.pallas_call(
        advance_kernel,
        grid_spec=pltpu.PrefetchScalarGridSpec(
            num_scalar_prefetch=2,
            grid=(count,),
            in_specs=[
                whole(cells, width), whole(8, cells), whole(8, cells), small, small, slab,
                pl.BlockSpec((radii, 8, width), lambda i, *_: (0, jnp.maximum(i * step - 1, 0), 0)),
                pl.BlockSpec((radii, 8, width), lambda i, *_: (0, jnp.minimum(i * step + step, ends), 0)),
                pl.BlockSpec((1, STRIP, width), lambda i, *_: (0, i, 0)),
                pl.BlockSpec((1, STRIP, width), lambda i, *_: (0, i, 0)),
                pl.BlockSpec((STRIP, 1), lambda i, *_: (i, 0)),
                pl.BlockSpec((STRIP, 1), lambda i, *_: (i, 0)),
            ],
            out_specs=slab,
            scratch_shapes=[
                pltpu.VMEM((cells + WINDOW, width), jnp.bfloat16),
                pltpu.VMEM((cells + WINDOW, width), jnp.bfloat16),
                pltpu.VMEM((points, width), jnp.float32),
            ],
        ),
        out_shape=f32(radii, meridian, width),
        name="advance",
    )(start, wins, stream, lax.ppermute(last, "ma", ma_up), lax.ppermute(first, "ma", ma_down),
      a.astype(jnp.float32), f, thermal, thermal, thermal, inner, outer,
      jnp.sin(angle)[:, None], jnp.cos(angle)[:, None])
    return thermal_later, pot_later


def solution(mesh):
    return jax.shard_map(
        per_device,
        mesh=mesh,
        in_specs=(
            P("row", None, "ma"),
            P("row", None),
            P("row", None),
            P("row", None),
            P(),
            P("row", "ma"),
        ),
        out_specs=(P("row", None, "ma"), P("row", "ma")),
        check_vma=False,
    )
```
